32 devices in a mesh: scan: 2 (over y), slab: 16 (over z, x, core).
Axes of the slice: x: 2, y: 2, z: 4, core: 2. Of those that a mesh axis runs over, the one named last changes fastest.
Arguments:
- image: float32 [2, 128, 256, 128], P(None, 'slab', 'scan'), parts along dimension 2, may hold values from -6 to 6
- sensitivity: bfloat16 [12, 2, 128, 128, 128], P('scan', None, 'slab'), parts along dimension 0, may hold values from -1.5 to 1.5
- kernel: float32 [256, 256, 256], P(None, 'slab'), may hold values from 0.1 to 4
Outputs:
- normal_image: float32 [2, 128, 256, 128], P(None, 'slab', 'scan'), parts along dimension 2
The draws below stay inside these ranges and needn't reach their ends.
There are 2 independent parts, one for each index of `scan`. The reference program is written for one: setup_inputs(seed, part) draws one part's arguments, and reference() takes and returns one part's arrays. A program takes and returns all parts, laid end to end along the dimension named above; an argument that names none is the same for every part. Nothing has to cross between parts.
All inputs are finite; a program needn't handle non-finite values.
Results may differ from the reference program's by a relative error of at most 0.0024.
Values may be sent and summed in bfloat16 or wider, within the bound.
A program may use at most 128 MiB of HBM per device.

```python
import math
import jax
import jax.numpy as jnp
from jax import lax

NX = 128
NY = 128
NZ = 128
COILS = 6
GX = 256
GY = 256
GZ = 256


def block_levels(key, shape, pieces, smallest, top_value):
    level, own = 1.0, jax.random.fold_in(key, 6)
    for dim, shards_of in pieces:
        draws = jnp.exp(jax.random.uniform(jax.random.fold_in(own, dim), (shards_of,), jnp.float32, smallest / len(pieces), top_value / len(pieces)))
        level = level * jnp.repeat(draws, shape[dim] // shards_of).reshape([-1 if axis == dim else 1 for axis in range(len(shape))])
    return level


def gaussian(own_key, extent, deviation, bound, cuts=(), held_as=jnp.bfloat16):
    values = deviation * jax.random.normal(own_key, extent, jnp.float32)
    if cuts:
        values = values * block_levels(own_key, extent, cuts, -0.22, 0.18)
    return jnp.clip(values, -bound, bound).astype(held_as)


def setup_inputs(seed: int = 0, part: int = 0) -> dict:
    streams_of = jax.random.split(jax.random.key(seed), 4)
    part_splits = jax.random.split(jax.random.fold_in(streams_of[3], part), 4)
    return {
        "image": gaussian(part_splits[0], (2, NX, NY, NZ), 1.0, 6.0, ((1, 16),), jnp.float32),
        "sensitivity": gaussian(part_splits[1], (COILS, 2, NX, NY, NZ), 0.25, 1.5, ((2, 16),)),
        "kernel": jnp.clip(jnp.exp(math.log(4.0) - 3.6888794 * jax.random.uniform(streams_of[2], (GX, GY, GZ), jnp.float32) ** block_levels(streams_of[2], (GX, GY, GZ), ((1, 16),), -0.2, 0.2)), 0.1, 4.0),
    }


smooth_weight = 0.1

def fourier_table(count_out, count_in, length, sign_value):
    row_index = lax.broadcasted_iota(jnp.int32, (count_out, count_in), 0)
    column_index = lax.broadcasted_iota(jnp.int32, (count_out, count_in), 1)
    phases = row_index * column_index % length
    angles = phases.astype(jnp.float32) * (2.0 * math.pi / length)
    factor = 1.0 / math.sqrt(length)
    real_part = jnp.cos(angles) * factor
    imaginary = sign_value * jnp.sin(angles) * factor
    stacked = jnp.stack([jnp.stack([real_part, -imaginary]), jnp.stack([imaginary, real_part])])
    return stacked.astype(jnp.bfloat16)

def transform(matrix, values, pattern):
    return jnp.einsum(pattern, matrix.astype(jnp.float32), values.astype(jnp.float32))

def reference(image, sensitivity, kernel):
    forward_first = fourier_table(GX, NX, GX, -1.0)
    forward_second = fourier_table(GY, NY, GY, -1.0)
    forward_third = fourier_table(GZ, NZ, GZ, -1.0)
    inverse_first = fourier_table(NX, GX, GX, 1.0)
    inverse_second = fourier_table(NY, GY, GY, 1.0)
    inverse_third = fourier_table(NZ, GZ, GZ, 1.0)

    def one_coil(accumulated, coil_maps):
        coil_real = coil_maps[0].astype(jnp.float32)
        coil_imaginary = coil_maps[1].astype(jnp.float32)
        coil_image = jnp.stack([coil_real * image[0] - coil_imaginary * image[1], coil_real * image[1] + coil_imaginary * image[0]]).astype(jnp.bfloat16)
        along_second = transform(forward_second, coil_image, 'pqkj,qajb->pakb').astype(jnp.bfloat16)
        along_third = transform(forward_third, along_second, 'pqkj,qabj->pabk').astype(jnp.bfloat16)
        spectrum = transform(forward_first, along_third, 'pqkj,qjab->pkab')
        filtered = (spectrum * kernel).astype(jnp.bfloat16)
        back_first = transform(inverse_first, filtered, 'pqkj,qjab->pkab').astype(jnp.bfloat16)
        back_third = transform(inverse_third, back_first, 'pqkj,qabj->pabk').astype(jnp.bfloat16)
        coil_result = transform(inverse_second, back_third, 'pqkj,qajb->pakb')
        accumulated = accumulated + jnp.stack([coil_real * coil_result[0] + coil_imaginary * coil_result[1], coil_real * coil_result[1] - coil_imaginary * coil_result[0]])
        return (accumulated, None)
    accumulated = lax.scan(one_coil, jnp.zeros(image.shape, jnp.float32), sensitivity)[0]
    padded = jnp.pad(image, ((0, 0), (1, 1), (1, 1), (1, 1)))
    beside = padded[:, 2:, 1:-1, 1:-1] + padded[:, :-2, 1:-1, 1:-1]
    beside = beside + padded[:, 1:-1, 2:, 1:-1] + padded[:, 1:-1, :-2, 1:-1]
    beside = beside + padded[:, 1:-1, 1:-1, 2:] + padded[:, 1:-1, 1:-1, :-2]
    penalty = 6.0 * image - beside
    return accumulated + smooth_weight * penalty
```

```python
import functools
import math

import jax
import jax.numpy as jnp
import numpy as np
from jax import lax
from jax.experimental import pallas as pl
from jax.experimental.pallas import tpu as pltpu
from jax.sharding import PartitionSpec as P

MESH = pl.DeviceIdType.MESH
smooth_weight = 0.1
F32 = jnp.float32
BF16 = jnp.bfloat16


def factor(count_out, count_in, length, sign_value):
    phases = np.outer(np.arange(count_out), np.arange(count_in)) % length
    angles = phases * (2.0 * math.pi / length)
    scale = 1.0 / math.sqrt(length)
    real, imag = np.cos(angles) * scale, sign_value * np.sin(angles) * scale
    return np.block([[real, -imag], [imag, real]]).astype(jnp.bfloat16)


def dot(a, b):
    return jnp.dot(a, b, preferred_element_type=F32)


def shifted(cells, step, axis):
    count = cells.shape[axis]
    index = lax.broadcasted_iota(jnp.int32, cells.shape, axis)
    edge = 0 if step == 1 else count - 1
    return jnp.where(index == edge, 0.0, pltpu.roll(cells, step % count, axis))


def kernel_body(
    n, image, sens, weight, fy, fzt, fx, hx, hzt, hy, out,
    sent, got, back, home, rows, halo, filt,
    send1, recv1, send2, recv2, hsend, hrecv, wsem,
):
    me = lax.axis_index("slab")
    coils, _, xs, ny, nz = sens.shape
    gx, gz = fx.shape[0] // 2, weight.shape[1]
    nx, gy = n * xs, fy.shape[0] // 2
    kys = gy // n
    part = kys * xs
    pair = 16 // xs

    columns = [
        pltpu.make_async_copy(weight.at[:, pl.ds(i * 128, 128)], filt.at[i], wsem.at[i])
        for i in range(gz // 128)
    ]
    for copy in columns:
        copy.start()

    barrier = pltpu.get_barrier_semaphore()

    @pl.loop(1, n)
    def _(k):
        pl.semaphore_signal(barrier, inc=1, device_id={"slab": lax.rem(me + k, n)}, device_id_type=MESH)

    pl.semaphore_wait(barrier, n - 1)

    def halo_copy(p, side):
        plane = xs - 1 if side == 0 else 0
        to = me + 1 if side == 0 else me - 1
        return pltpu.make_async_remote_copy(
            src_ref=image.at[p, plane], dst_ref=halo.at[side, p],
            send_sem=hsend.at[side, p], recv_sem=hrecv.at[side, p],
            device_id={"slab": lax.rem(to + n, n)}, device_id_type=MESH)

    def exchange(source, target, c, k, send_sem, recv_sem):
        to = lax.rem(me + k, n)
        return pltpu.make_async_remote_copy(
            src_ref=source.at[c, to], dst_ref=target.at[c, me],
            send_sem=send_sem.at[c, to], recv_sem=recv_sem.at[c, me],
            device_id={"slab": to}, device_id_type=MESH)

    def arrival(source, target, c, k, send_sem, recv_sem):
        owner = lax.rem(me + k, n)
        return pltpu.make_async_remote_copy(
            src_ref=source.at[c, owner], dst_ref=target.at[c, owner],
            send_sem=send_sem.at[c, owner], recv_sem=recv_sem.at[c, owner],
            device_id={"slab": owner}, device_id_type=MESH)

    def start_all(source, target, c, send_sem, recv_sem):
        @pl.loop(1, n)
        def _(k):
            exchange(source, target, c, k, send_sem, recv_sem).start()

        target[c, me] = source[c, me]

    def wait_all(source, target, c, send_sem, recv_sem):
        @pl.loop(1, n)
        def _(k):
            arrival(source, target, c, k, send_sem, recv_sem).wait_recv()

    def drain(source, target, c, send_sem, recv_sem):
        @pl.loop(1, n)
        def _(k):
            exchange(source, target, c, k, send_sem, recv_sem).wait_send()

    @pl.loop(0, coils)
    def _(c):
        @pl.loop(0, xs // 2)
        def _(h):
            halves = []
            for j in range(2):
                x = 2 * h + j
                cr, ci = sens[c, 0, x].astype(F32), sens[c, 1, x].astype(F32)
                vr, vi = image[0, x], image[1, x]
                halves.append(jnp.concatenate([cr * vr - ci * vi, cr * vi + ci * vr], axis=0).astype(BF16))
            lines = dot(fy[...], jnp.concatenate(halves, axis=1))
            for j in range(2):
                rows[pl.ds(2 * h + j, 2 * gy, stride=xs), :] = lines[:, j * nz:(j + 1) * nz]

        for q in range(2):
            size = gy * xs
            sent[c, :, q * part:(q + 1) * part, :] = (
                rows[q * size:(q + 1) * size, :].reshape(n, part, nz).astype(BF16))
        start_all(sent, got, c, send1, recv1)

        @pl.when(c == 0)
        def _():
            @pl.when(me < n - 1)
            def _():
                for p in range(2):
                    halo_copy(p, 0).start()

            @pl.when(me > 0)
            def _():
                for p in range(2):
                    halo_copy(p, 1).start()

    for copy in columns:
        copy.wait()

    @pl.loop(0, coils)
    def _(c):
        wait_all(sent, got, c, send1, recv1)

        @pl.loop(0, kys // pair)
        def _(kp):
            base = pl.multiple_of(kp * 16, 16)
            cells = [got[c, :, pl.ds(q * part + base, 16), :].reshape(n * 16, nz) for q in range(2)]
            third = dot(jnp.concatenate(cells, axis=1), fzt[...]).reshape(n, pair, xs, 2 * gz)
            results = []
            for j in range(pair):
                b = third[:, j].reshape(nx, 2 * gz).astype(BF16)
                spectrum = dot(fx[...], jnp.concatenate([b[:, :gz], b[:, gz:]], axis=0))
                k = jnp.concatenate(
                    [filt[i, pl.ds(kp * pair + j, gx, stride=kys), :] for i in range(gz // 128)], axis=1)
                filtered = jnp.concatenate([spectrum[:gx] * k, spectrum[gx:] * k], axis=0).astype(BF16)
                first = dot(hx[...], filtered).astype(BF16)
                results.append(dot(jnp.concatenate([first[:nx], first[nx:]], axis=1), hzt[...]))
            for q in range(2):
                parts = [r[:, q * nz:(q + 1) * nz].reshape(n, 1, xs, nz) for r in results]
                back[c, :, pl.ds(q * part + base, 16), :] = (
                    jnp.concatenate(parts, axis=1).reshape(n, 16, nz).astype(BF16))

        start_all(back, home, c, send2, recv2)

    @pl.when(me < n - 1)
    def _():
        for p in range(2):
            halo_copy(p, 0).wait_send()
            halo_copy(p, 1).wait_recv()

    @pl.when(me > 0)
    def _():
        for p in range(2):
            halo_copy(p, 1).wait_send()
            halo_copy(p, 0).wait_recv()

    for p in range(2):
        for x in range(xs):
            here = image[p, x]
            if x == 0:
                before = jnp.where(me > 0, halo[0, p], 0.0)
            else:
                before = image[p, x - 1]
            if x == xs - 1:
                after = jnp.where(me < n - 1, halo[1, p], 0.0)
            else:
                after = image[p, x + 1]
            beside = before + after
            for axis in range(2):
                beside = beside + shifted(here, 1, axis) + shifted(here, -1, axis)
            out[p, x] = smooth_weight * (6.0 * here - beside)

    @pl.loop(0, coils)
    def _(c):
        wait_all(back, home, c, send2, recv2)
        size = gy * xs
        for q in range(2):
            rows[q * size:(q + 1) * size, :] = home[c, :, q * part:(q + 1) * part, :].reshape(size, nz).astype(F32)

        @pl.loop(0, xs // 2)
        def _(h):
            lines = [rows[pl.ds(2 * h + j, 2 * gy, stride=xs), :] for j in range(2)]
            cells = dot(hy[...], jnp.concatenate(lines, axis=1).astype(BF16))
            for j in range(2):
                x = 2 * h + j
                re, im = cells[:ny, j * nz:(j + 1) * nz], cells[ny:, j * nz:(j + 1) * nz]
                cr, ci = sens[c, 0, x].astype(F32), sens[c, 1, x].astype(F32)
                out[0, x] = out[0, x] + cr * re + ci * im
                out[1, x] = out[1, x] + cr * im - ci * re

    @pl.loop(0, coils)
    def _(c):
        drain(sent, got, c, send1, recv1)
        drain(back, home, c, send2, recv2)


def fused(n, image, sensitivity, kernel):
    coils, _, xs, ny, nz = sensitivity.shape
    gx, kys, gz = kernel.shape
    nx, gy = n * xs, n * kys
    block = (coils, n, 2 * kys * xs, nz)
    tables = (
        factor(gy, ny, gy, -1.0),
        factor(gz, nz, gz, -1.0).T,
        factor(gx, nx, gx, -1.0),
        factor(nx, gx, gx, 1.0),
        factor(nz, gz, gz, 1.0).T,
        factor(ny, gy, gy, 1.0),
    )
    vmem = pl.BlockSpec(memory_space=pltpu.VMEM)
    dma = pltpu.SemaphoreType.DMA
    return pl.pallas_call(
        functools.partial(kernel_body, n),
        out_shape=jax.ShapeDtypeStruct(image.shape, F32),
        in_specs=[vmem] * 2 + [pl.BlockSpec(memory_space=pl.ANY)] + [vmem] * 6,
        out_specs=vmem,
        scratch_shapes=[pltpu.VMEM(block, BF16)] * 4
        + [pltpu.VMEM((2 * gy * xs, nz), F32), pltpu.VMEM((2, 2, ny, nz), F32),
           pltpu.VMEM((gz // 128, gx * kys, 128), F32)]
        + [dma((coils, n))] * 4 + [dma((2, 2))] * 2 + [dma((gz // 128,))],
        compiler_params=pltpu.CompilerParams(
            collective_id=0, has_side_effects=True, vmem_limit_bytes=62 * 2**20),
    )(image, sensitivity, kernel.reshape(gx * kys, gz), *[jnp.asarray(t) for t in tables])


def with_halo(cells, axis, dim):
    count = lax.axis_size(axis)
    head = lax.slice_in_dim(cells, 0, 1, axis=dim)
    tail = lax.slice_in_dim(cells, cells.shape[dim] - 1, cells.shape[dim], axis=dim)
    return jnp.concatenate(
        [
            lax.ppermute(tail, axis, [(i, i + 1) for i in range(count - 1)]),
            cells,
            lax.ppermute(head, axis, [(i + 1, i) for i in range(count - 1)]),
        ],
        axis=dim,
    )


def staged(n, image, sensitivity, kernel):
    coils, _, xs, ny, nz = sensitivity.shape
    gx, kys, gz = kernel.shape
    nx, gy = n * xs, n * kys

    def table(count_out, count_in, length, sign_value):
        both = factor(count_out, count_in, length, sign_value)
        return jnp.asarray(both.reshape(2, count_out, 2, count_in).transpose(0, 2, 1, 3))

    def apply(matrix, values, pattern):
        return jnp.einsum(pattern, matrix, values, preferred_element_type=F32)

    real, imag = sensitivity[:, 0].astype(F32), sensitivity[:, 1].astype(F32)
    images = jnp.stack(
        [real * image[0] - imag * image[1], real * image[1] + imag * image[0]], axis=1).astype(BF16)
    second = apply(table(gy, ny, gy, -1.0), images, "pqkj,cqajb->cpakb").astype(BF16)
    second = lax.all_to_all(second, "slab", split_axis=3, concat_axis=2, tiled=True)
    third = apply(table(gz, nz, gz, -1.0), second, "pqkj,cqabj->cpabk").astype(BF16)
    spectrum = apply(table(gx, nx, gx, -1.0), third, "pqkj,cqjab->cpkab")
    filtered = (spectrum * kernel).astype(BF16)
    first = apply(table(nx, gx, gx, 1.0), filtered, "pqkj,cqjab->cpkab").astype(BF16)
    back = apply(table(nz, gz, gz, 1.0), first, "pqkj,cqabj->cpabk").astype(BF16)
    back = lax.all_to_all(back, "slab", split_axis=2, concat_axis=3, tiled=True)
    cells = apply(table(ny, gy, gy, 1.0), back, "pqkj,cqajb->cpakb")
    summed = jnp.stack([
        jnp.sum(real * cells[:, 0] + imag * cells[:, 1], axis=0),
        jnp.sum(real * cells[:, 1] - imag * cells[:, 0], axis=0)])
    padded = with_halo(image.astype(BF16), "slab", 1).astype(image.dtype)
    beside = padded[:, 2:] + padded[:, :-2]
    wide = jnp.pad(image, ((0, 0), (0, 0), (1, 1), (1, 1)))
    beside = beside + wide[:, :, 2:, 1:-1] + wide[:, :, :-2, 1:-1]
    beside = beside + wide[:, :, 1:-1, 2:] + wide[:, :, 1:-1, :-2]
    return summed + smooth_weight * (6.0 * image - beside)


def solution(mesh):
    n = mesh.shape["slab"]

    def local(image, sensitivity, kernel):
        tiled = sensitivity.shape[2] == 8 and kernel.shape[1] % 2 == 0
        form = fused if tiled else staged
        return form(n, image, sensitivity, kernel)

    return jax.shard_map(
        local,
        mesh=mesh,
        in_specs=(
            P(None, "slab", "scan", None),
            P("scan", None, "slab", None, None),
            P(None, "slab", None),
        ),
        out_specs=P(None, "slab", "scan", None),
        check_vma=False,
    )
```

```python
import functools
import math

import jax
import jax.numpy as jnp
import numpy as np
from jax import lax
from jax.experimental import pallas as pl
from jax.experimental.pallas import tpu as pltpu
from jax.sharding import PartitionSpec as P

MESH = pl.DeviceIdType.MESH
smooth_weight = 0.1
F32 = jnp.float32
BF16 = jnp.bfloat16


def factor(count_out, count_in, length, sign_value):
    phases = np.outer(np.arange(count_out), np.arange(count_in)) % length
    angles = phases * (2.0 * math.pi / length)
    scale = 1.0 / math.sqrt(length)
    real, imag = np.cos(angles) * scale, sign_value * np.sin(angles) * scale
    return np.block([[real, -imag], [imag, real]]).astype(jnp.bfloat16)


def dot(a, b):
    return jnp.dot(a, b, preferred_element_type=F32)


def shifted(cells, step, axis):
    count = cells.shape[axis]
    index = lax.broadcasted_iota(jnp.int32, cells.shape, axis)
    edge = 0 if step == 1 else count - 1
    return jnp.where(index == edge, 0.0, pltpu.roll(cells, step % count, axis))


def kernel_body(
    n, image, sens, weight, fy, fzt, fx, hx, hzt, hy, out,
    sent, got, back, home, rows, halo, filt,
    other_sens, mine, other_image, other_out, total, other_total,
    send1, recv1, send2, recv2, hsend, hrecv, wsem, psend, precv, tsend, trecv,
):
    me = lax.axis_index("slab")
    coils, _, xs, ny, nz = sens.shape
    gx, gz = fx.shape[0] // 2, weight.shape[1]
    nx, gy = n * xs, fy.shape[0] // 2
    kys = gy // n
    part = kys * xs
    pair = 16 // xs
    nh = n // 2
    half, place = me // nh, lax.rem(me, nh)
    far = lax.rem(me + nh, n)
    far_half = 1 - half
    mid = coils // 2

    columns = [
        pltpu.make_async_copy(weight.at[:, pl.ds(i * 128, 128)], filt.at[i], wsem.at[i])
        for i in range(gz // 128)
    ]
    for copy in columns:
        copy.start()

    barrier = pltpu.get_barrier_semaphore()

    @pl.loop(1, n)
    def _(k):
        pl.semaphore_signal(barrier, inc=1, device_id={"slab": lax.rem(me + k, n)}, device_id_type=MESH)

    pl.semaphore_wait(barrier, n - 1)

    def halo_copy(p, side):
        plane = xs - 1 if side == 0 else 0
        to = me + 1 if side == 0 else me - 1
        return pltpu.make_async_remote_copy(
            src_ref=image.at[p, plane], dst_ref=halo.at[side, p],
            send_sem=hsend.at[side, p], recv_sem=hrecv.at[side, p],
            device_id={"slab": lax.rem(to + n, n)}, device_id_type=MESH)

    def to_far(source, target, send_sem, recv_sem):
        return pltpu.make_async_remote_copy(
            src_ref=source, dst_ref=target, send_sem=send_sem, recv_sem=recv_sem,
            device_id={"slab": far}, device_id_type=MESH)

    def maps(c):
        return to_far(sens.at[c], other_sens.at[c], psend.at[c], precv.at[c])

    image_copy = to_far(mine, other_image, tsend.at[0], trecv.at[0])
    total_copy = to_far(total, other_total, tsend.at[1], trecv.at[1])

    def block(source, target, c, to, slot, landing, send_sem, recv_sem):
        return pltpu.make_async_remote_copy(
            src_ref=source.at[c, slot], dst_ref=target.at[c, landing],
            send_sem=send_sem.at[c, slot], recv_sem=recv_sem.at[c, landing],
            device_id={"slab": to}, device_id_type=MESH)

    def over_all(source, target, c, send_sem, recv_sem, action):
        @pl.loop(1, n)
        def _(k):
            to = lax.rem(me + k, n)
            landing = to if action == "recv" else me
            act(block(source, target, c, to, to, landing, send_sem, recv_sem), action)

    def over_half(source, target, c, send_sem, recv_sem, action):
        @pl.loop(1, nh)
        def _(k):
            near = lax.rem(place + k, nh)
            for g in range(2):
                landing = near if action == "recv" else place
                act(block(source, target, c, half * nh + near, g * nh + near, g * nh + landing,
                          send_sem, recv_sem), action)

    def act(copy, action):
        if action == "start":
            copy.start()
        elif action == "recv":
            copy.wait_recv()
        else:
            copy.wait_send()

    def is_split(c):
        return lax.rem(c, mid) != 0

    def either(c, first, second):
        pl.when(is_split(c))(first)
        pl.when(jnp.logical_not(is_split(c)))(second)

    def traffic(source, target, c, send_sem, recv_sem, action):
        either(c,
               lambda: over_half(source, target, c, send_sem, recv_sem, action),
               lambda: over_all(source, target, c, send_sem, recv_sem, action))

    def start_all(source, target, c, send_sem, recv_sem):
        over_all(source, target, c, send_sem, recv_sem, "start")
        target[c, me] = source[c, me]

    def start_half(source, target, c, send_sem, recv_sem):
        over_half(source, target, c, send_sem, recv_sem, "start")
        for g in range(2):
            target[c, g * nh + place] = source[c, g * nh + place]

    def along_second(table, maps_of, cells_of):
        count = table.shape[0]

        @pl.loop(0, xs // 2)
        def _(h):
            halves = []
            for j in range(2):
                x = 2 * h + j
                cr, ci = maps_of(0, x).astype(F32), maps_of(1, x).astype(F32)
                vr, vi = cells_of(0, x).astype(F32), cells_of(1, x).astype(F32)
                halves.append(jnp.concatenate([cr * vr - ci * vi, cr * vi + ci * vr], axis=0).astype(BF16))
            lines = dot(table, jnp.concatenate(halves, axis=1))
            for j in range(2):
                rows[pl.ds(2 * h + j, count, stride=xs), :] = lines[:, j * nz:(j + 1) * nz]

    def forward_all(c):
        along_second(fy[...], lambda p, x: sens[c, p, x], lambda p, x: image[p, x])
        size = gy * xs
        for q in range(2):
            sent[c, :, q * part:(q + 1) * part, :] = (
                rows[q * size:(q + 1) * size, :].reshape(n, part, nz).astype(BF16))
        start_all(sent, got, c, send1, recv1)

    gh = gy // 2

    def forward_half(c):
        maps(c).wait_recv()
        table = jnp.concatenate(
            [fy[pl.ds(pl.multiple_of(q * gy + half * gh, gh), gh), :] for q in range(2)], axis=0)
        size = gh * xs
        for own in (True, False):
            if own:
                along_second(table, lambda p, x: sens[c, p, x], lambda p, x: image[p, x])
            else:
                along_second(table, lambda p, x: other_sens[c, p, x], lambda p, x: other_image[p, x])
            start = (half if own else far_half) * nh
            for q in range(2):
                sent[c, pl.ds(start, nh), q * part:(q + 1) * part, :] = (
                    rows[q * size:(q + 1) * size, :].reshape(nh, part, nz).astype(BF16))
        start_half(sent, got, c, send1, recv1)

    def middle(c):
        @pl.loop(0, kys // pair)
        def _(kp):
            base = pl.multiple_of(kp * 16, 16)
            cells = [got[c, :, pl.ds(q * part + base, 16), :].reshape(n * 16, nz) for q in range(2)]
            third = dot(jnp.concatenate(cells, axis=1), fzt[...]).reshape(n, pair, xs, 2 * gz)
            results = []
            for j in range(pair):
                b = third[:, j].reshape(nx, 2 * gz).astype(BF16)
                spectrum = dot(fx[...], jnp.concatenate([b[:, :gz], b[:, gz:]], axis=0))
                k = jnp.concatenate(
                    [filt[i, pl.ds(kp * pair + j, gx, stride=kys), :] for i in range(gz // 128)], axis=1)
                filtered = jnp.concatenate([spectrum[:gx] * k, spectrum[gx:] * k], axis=0).astype(BF16)
                first = dot(hx[...], filtered).astype(BF16)
                results.append(dot(jnp.concatenate([first[:nx], first[nx:]], axis=1), hzt[...]))
            for q in range(2):
                parts = [r[:, q * nz:(q + 1) * nz].reshape(n, 1, xs, nz) for r in results]
                back[c, :, pl.ds(q * part + base, 16), :] = (
                    jnp.concatenate(parts, axis=1).reshape(n, 16, nz).astype(BF16))

    def gather(table, count, maps_of, acc):
        @pl.loop(0, xs // 2)
        def _(h):
            lines = [rows[pl.ds(2 * h + j, count, stride=xs), :] for j in range(2)]
            cells = dot(table, jnp.concatenate(lines, axis=1).astype(BF16))
            for j in range(2):
                x = 2 * h + j
                re, im = cells[:ny, j * nz:(j + 1) * nz], cells[ny:, j * nz:(j + 1) * nz]
                cr, ci = maps_of(0, x).astype(F32), maps_of(1, x).astype(F32)
                acc[0, x] = acc[0, x] + cr * re + ci * im
                acc[1, x] = acc[1, x] + cr * im - ci * re

    def inverse_all(c):
        over_all(back, home, c, send2, recv2, "recv")
        size = gy * xs
        for q in range(2):
            rows[q * size:(q + 1) * size, :] = home[c, :, q * part:(q + 1) * part, :].reshape(size, nz).astype(F32)
        gather(hy[...], 2 * gy, lambda p, x: sens[c, p, x], out)

    def inverse_half(c):
        over_half(back, home, c, send2, recv2, "recv")
        table = jnp.concatenate(
            [hy[:, pl.ds(pl.multiple_of(q * gy + half * gh, gh), gh)] for q in range(2)], axis=1)
        size = gh * xs
        for own in (False, True):
            start = (half if own else far_half) * nh
            for q in range(2):
                rows[q * size:(q + 1) * size, :] = (
                    home[c, pl.ds(start, nh), q * part:(q + 1) * part, :].reshape(size, nz).astype(F32))
            if own:
                gather(table, 2 * gh, lambda p, x: sens[c, p, x], out)
            else:
                gather(table, 2 * gh, lambda p, x: other_sens[c, p, x], other_out)

    mine[...] = image[...].astype(BF16)
    maps(1).start()
    image_copy.start()
    forward_all(0)
    maps(2).start()

    @pl.when(me < n - 1)
    def _():
        for p in range(2):
            halo_copy(p, 0).start()

    @pl.when(me > 0)
    def _():
        for p in range(2):
            halo_copy(p, 1).start()

    other_out[...] = jnp.zeros_like(other_out)
    out[...] = jnp.zeros_like(out)
    image_copy.wait_recv()
    forward_half(1)
    for copy in columns:
        copy.wait()

    @pl.loop(0, coils)
    def _(c):
        @pl.when(c < mid - 1)
        def _():
            maps(c + mid + 1).start()

        @pl.when(c == 0)
        def _():
            forward_half(2)
            forward_all(mid)

        @pl.when(jnp.logical_and(c > 0, c < mid))
        def _():
            forward_half(c + mid)

        traffic(sent, got, c, send1, recv1, "recv")
        middle(c)
        either(c,
               lambda: start_half(back, home, c, send2, recv2),
               lambda: start_all(back, home, c, send2, recv2))

        @pl.when(jnp.logical_and(c >= mid, c < coils - 1))
        def _():
            inverse_half(c - mid + 1)

    @pl.loop(mid + 1, coils)
    def _(c):
        inverse_half(c)

    total[...] = other_out[...].astype(BF16)
    total_copy.start()
    inverse_all(0)

    @pl.when(me < n - 1)
    def _():
        for p in range(2):
            halo_copy(p, 0).wait_send()
            halo_copy(p, 1).wait_recv()

    @pl.when(me > 0)
    def _():
        for p in range(2):
            halo_copy(p, 1).wait_send()
            halo_copy(p, 0).wait_recv()

    for p in range(2):
        for x in range(xs):
            here = image[p, x]
            if x == 0:
                before = jnp.where(me > 0, halo[0, p], 0.0)
            else:
                before = image[p, x - 1]
            if x == xs - 1:
                after = jnp.where(me < n - 1, halo[1, p], 0.0)
            else:
                after = image[p, x + 1]
            beside = before + after
            for axis in range(2):
                beside = beside + shifted(here, 1, axis) + shifted(here, -1, axis)
            out[p, x] = out[p, x] + smooth_weight * (6.0 * here - beside)

    inverse_all(mid)
    total_copy.wait_recv()
    out[...] = out[...] + other_total[...].astype(F32)

    @pl.loop(0, coils)
    def _(c):
        traffic(sent, got, c, send1, recv1, "send")
        traffic(back, home, c, send2, recv2, "send")

    @pl.loop(1, mid)
    def _(c):
        maps(c).wait_send()
        maps(c + mid).wait_send()

    image_copy.wait_send()
    total_copy.wait_send()


def fused(n, image, sensitivity, kernel):
    coils, _, xs, ny, nz = sensitivity.shape
    gx, kys, gz = kernel.shape
    nx, gy = n * xs, n * kys
    block = (coils, n, 2 * kys * xs, nz)
    tables = (
        factor(gy, ny, gy, -1.0),
        factor(gz, nz, gz, -1.0).T,
        factor(gx, nx, gx, -1.0),
        factor(nx, gx, gx, 1.0),
        factor(nz, gz, gz, 1.0).T,
        factor(ny, gy, gy, 1.0),
    )
    vmem = pl.BlockSpec(memory_space=pltpu.VMEM)
    dma = pltpu.SemaphoreType.DMA
    return pl.pallas_call(
        functools.partial(kernel_body, n),
        out_shape=jax.ShapeDtypeStruct(image.shape, F32),
        in_specs=[vmem] * 2 + [pl.BlockSpec(memory_space=pl.ANY)] + [vmem] * 6,
        out_specs=vmem,
        scratch_shapes=[pltpu.VMEM(block, BF16)] * 4
        + [pltpu.VMEM((2 * gy * xs, nz), F32), pltpu.VMEM((2, 2, ny, nz), F32),
           pltpu.VMEM((gz // 128, gx * kys, 128), F32)]
        + [pltpu.VMEM(sensitivity.shape, BF16)]
        + [pltpu.VMEM(image.shape, BF16)] * 2 + [pltpu.VMEM(image.shape, F32)]
        + [pltpu.VMEM(image.shape, BF16)] * 2
        + [dma((coils, n))] * 4 + [dma((2, 2))] * 2 + [dma((gz // 128,))]
        + [dma((coils,))] * 2 + [dma((2,))] * 2,
        compiler_params=pltpu.CompilerParams(
            collective_id=0, has_side_effects=True, vmem_limit_bytes=62 * 2**20),
    )(image, sensitivity, kernel.reshape(gx * kys, gz), *[jnp.asarray(t) for t in tables])


def with_halo(cells, axis, dim):
    count = lax.axis_size(axis)
    head = lax.slice_in_dim(cells, 0, 1, axis=dim)
    tail = lax.slice_in_dim(cells, cells.shape[dim] - 1, cells.shape[dim], axis=dim)
    return jnp.concatenate(
        [
            lax.ppermute(tail, axis, [(i, i + 1) for i in range(count - 1)]),
            cells,
            lax.ppermute(head, axis, [(i + 1, i) for i in range(count - 1)]),
        ],
        axis=dim,
    )


def staged(n, image, sensitivity, kernel):
    coils, _, xs, ny, nz = sensitivity.shape
    gx, kys, gz = kernel.shape
    nx, gy = n * xs, n * kys

    def table(count_out, count_in, length, sign_value):
        both = factor(count_out, count_in, length, sign_value)
        return jnp.asarray(both.reshape(2, count_out, 2, count_in).transpose(0, 2, 1, 3))

    def apply(matrix, values, pattern):
        return jnp.einsum(pattern, matrix, values, preferred_element_type=F32)

    real, imag = sensitivity[:, 0].astype(F32), sensitivity[:, 1].astype(F32)
    images = jnp.stack(
        [real * image[0] - imag * image[1], real * image[1] + imag * image[0]], axis=1).astype(BF16)
    second = apply(table(gy, ny, gy, -1.0), images, "pqkj,cqajb->cpakb").astype(BF16)
    second = lax.all_to_all(second, "slab", split_axis=3, concat_axis=2, tiled=True)
    third = apply(table(gz, nz, gz, -1.0), second, "pqkj,cqabj->cpabk").astype(BF16)
    spectrum = apply(table(gx, nx, gx, -1.0), third, "pqkj,cqjab->cpkab")
    filtered = (spectrum * kernel).astype(BF16)
    first = apply(table(nx, gx, gx, 1.0), filtered, "pqkj,cqjab->cpkab").astype(BF16)
    back = apply(table(nz, gz, gz, 1.0), first, "pqkj,cqabj->cpabk").astype(BF16)
    back = lax.all_to_all(back, "slab", split_axis=2, concat_axis=3, tiled=True)
    cells = apply(table(ny, gy, gy, 1.0), back, "pqkj,cqajb->cpakb")
    summed = jnp.stack([
        jnp.sum(real * cells[:, 0] + imag * cells[:, 1], axis=0),
        jnp.sum(real * cells[:, 1] - imag * cells[:, 0], axis=0)])
    padded = with_halo(image.astype(BF16), "slab", 1).astype(image.dtype)
    beside = padded[:, 2:] + padded[:, :-2]
    wide = jnp.pad(image, ((0, 0), (0, 0), (1, 1), (1, 1)))
    beside = beside + wide[:, :, 2:, 1:-1] + wide[:, :, :-2, 1:-1]
    beside = beside + wide[:, :, 1:-1, 2:] + wide[:, :, 1:-1, :-2]
    return summed + smooth_weight * (6.0 * image - beside)


def solution(mesh):
    n = mesh.shape["slab"]

    def local(image, sensitivity, kernel):
        tiled = sensitivity.shape[2] == 8 and kernel.shape[1] % 2 == 0 and n % 2 == 0 and sensitivity.shape[0] == 6
        form = fused if tiled else staged
        return form(n, image, sensitivity, kernel)

    return jax.shard_map(
        local,
        mesh=mesh,
        in_specs=(
            P(None, "slab", "scan", None),
            P("scan", None, "slab", None, None),
            P(None, "slab", None),
        ),
        out_specs=P(None, "slab", "scan", None),
        check_vma=False,
    )
```
